32 devices in a mesh: replica: 2 (over x), fsdp: 16 (over z, y, core).
Axes of the slice: x: 2, y: 2, z: 4, core: 2. Of those that a mesh axis runs over, the one named last changes fastest.
Arguments:
- tokens: bfloat16 [16384, 1152], P(('replica', 'fsdp')), may hold values from -6 to 6
- cotangent: bfloat16 [16384, 1152], P(('replica', 'fsdp')), may hold values from -6 to 6
- piece_starts: int32 [32, 1], P(('replica', 'fsdp')), may hold values from 0 to 256, as said below
- w_query: bfloat16 [1152, 1024], P('fsdp'), may hold values from -0.1875 to 0.1875
- w_key: bfloat16 [1152, 256], P('fsdp'), may hold values from -0.1875 to 0.1875
- w_value: bfloat16 [1152, 256], P('fsdp'), may hold values from -0.1875 to 0.1875
- w_out: bfloat16 [1024, 1152], P('fsdp'), may hold values from -0.1875 to 0.1875
- w_gate: bfloat16 [1152, 6912], P('fsdp'), may hold values from -0.1875 to 0.1875
- w_up: bfloat16 [1152, 6912], P('fsdp'), may hold values from -0.1875 to 0.1875
- w_down: bfloat16 [6912, 1152], P('fsdp'), may hold values from -0.078125 to 0.078125
- attn_pre_gain: bfloat16 [1152], P('fsdp'), may hold values from 0.5 to 1.5
- query_gain: bfloat16 [256], P('fsdp'), may hold values from 1 to 2.5
- key_gain: bfloat16 [256], P('fsdp'), may hold values from 0.25 to 1.75
- attn_post_gain: bfloat16 [1152], P('fsdp'), may hold values from 0.25 to 1.75
- mlp_pre_gain: bfloat16 [1152], P('fsdp'), may hold values from 0.5 to 1.5
- mlp_post_gain: bfloat16 [1152], P('fsdp'), may hold values from 0.25 to 1.75
Outputs:
- layer_out: bfloat16 [16384, 1152], P(('replica', 'fsdp'))
- input_grad: float32 [16384, 1152], P(('replica', 'fsdp'))
- grad_query: float32 [1152, 1024], P('fsdp')
- grad_key: float32 [1152, 256], P('fsdp')
- grad_value: float32 [1152, 256], P('fsdp')
- grad_out: float32 [1024, 1152], P('fsdp')
- grad_gate: float32 [1152, 6912], P('fsdp')
- grad_up: float32 [1152, 6912], P('fsdp')
- grad_down: float32 [6912, 1152], P('fsdp')
- grad_attn_pre: float32 [1152], P('fsdp')
- grad_query_gain: float32 [256], P('fsdp')
- grad_key_gain: float32 [256], P('fsdp')
- grad_attn_post: float32 [1152], P('fsdp')
- grad_mlp_pre: float32 [1152], P('fsdp')
- grad_mlp_post: float32 [1152], P('fsdp')
The draws below stay inside these ranges and needn't reach their ends.
Inputs may be any that keep to these rules, and one draw needn't show every extreme that they name: `piece_starts`: each row holds the starts of the 1 image pieces of 256 tokens in one sequence, rising, the pieces disjoint and within the sequence's 512 tokens; the other tokens of the sequence are causal text.
All inputs are finite; a program needn't handle non-finite values.
Results may differ from the reference program's by a relative error of at most 0.018.
Values may be sent and summed in bfloat16 or wider, within the bound.
A program may use at most 320 MiB of HBM per device.

```python
import math
import jax
import jax.numpy as jnp
from jax import lax

D = 1152
H = 4
HD = 256
FF = 6912
TOK_DEV = 512
PIECE = 256
NPIECE = 1
SEQS = 32
TOKENS = 16384


def draw_piece_starts(key, part):
    slack = TOK_DEV - NPIECE * PIECE
    raw = jax.random.randint(jax.random.fold_in(key, 7), (SEQS, NPIECE), 0, 1 << 20)
    row = jnp.arange(SEQS, dtype=jnp.int32)
    remaining = jnp.full((SEQS,), slack, jnp.int32)
    offset = jnp.zeros((SEQS,), jnp.int32)
    columns = []
    for piece in range(NPIECE):
        chosen = raw[:, piece] % (remaining + 1)
        if piece == NPIECE - 1:
            chosen = jnp.where(row == 0, remaining, chosen)
        chosen = jnp.where(row == 1, 0, chosen)
        offset = offset + chosen
        remaining = remaining - chosen
        columns.append(offset + piece * PIECE)
    return jnp.stack(columns, axis=1).astype(jnp.int32)


def levels(stream_key, shape, shards, low, top_value):
    level = 1.0
    for position, blocks in shards:
        heights = jax.random.uniform(jax.random.fold_in(jax.random.fold_in(stream_key, 6), position), (blocks,), jnp.float32, low / len(shards), top_value / len(shards))
        level = level * jnp.repeat(jnp.exp(heights), shape[position] // blocks).reshape((-1,) + (1,) * (len(shape) - 1 - position))
    return level


def centred(key, extent, scale, limit, pieces=(), held_as=jnp.bfloat16):
    array = jax.random.normal(key, extent, jnp.float32) * scale
    if len(pieces) > 0:
        array = levels(key, extent, pieces, -0.22, 0.18) * array
    return jnp.clip(array, min=-limit, max=limit).astype(held_as)


def setup_inputs(seed: int = 0) -> dict:
    splits = jax.random.split(jax.random.key(seed), 17)
    tokens = centred(splits[0], (TOKENS, D), 1.0, 6.0, ((0, 32),))
    cotangent = centred(splits[1], (TOKENS, D), 1.0, 6.0, ((0, 32),))
    piece_starts = draw_piece_starts(jax.random.fold_in(splits[16], 71), 0)
    w_query = centred(splits[3], (D, H * HD), D ** -0.5, 0.1875, ((0, 16),))
    w_key = centred(splits[4], (D, HD), D ** -0.5, 0.1875, ((0, 16),))
    w_value = centred(splits[5], (D, HD), D ** -0.5, 0.1875, ((0, 16),))
    w_out = centred(splits[6], (H * HD, D), (H * HD) ** -0.5, 0.1875, ((0, 16),))
    w_gate = centred(splits[7], (D, FF), D ** -0.5, 0.1875, ((0, 16),))
    w_up = centred(splits[8], (D, FF), D ** -0.5, 0.1875, ((0, 16),))
    w_down = centred(splits[9], (FF, D), FF ** -0.5, 0.078125, ((0, 16),))
    attn_pre_gain = jnp.clip(1.0 + 0.1 * jax.random.normal(splits[10], (D,), jnp.float32), 0.5, 1.5).astype(jnp.bfloat16)
    query_gain = jnp.clip(jnp.exp(math.log(2.5) - 0.916290732 * jax.random.uniform(splits[11], (HD,), jnp.float32) ** levels(splits[11], (HD,), ((0, 16),), -0.2, 0.2)), 1.0, 2.5).astype(jnp.bfloat16)
    key_gain = jnp.clip(1.0 + 0.15 * jax.random.normal(splits[12], (HD,), jnp.float32), 0.25, 1.75).astype(jnp.bfloat16)
    attn_post_gain = jnp.clip(1.0 + 0.15 * jax.random.normal(splits[13], (D,), jnp.float32), 0.25, 1.75).astype(jnp.bfloat16)
    mlp_pre_gain = jnp.clip(1.0 + 0.1 * jax.random.normal(splits[14], (D,), jnp.float32), 0.5, 1.5).astype(jnp.bfloat16)
    mlp_post_gain = jnp.clip(1.0 + 0.15 * jax.random.normal(splits[15], (D,), jnp.float32), 0.25, 1.75).astype(jnp.bfloat16)
    return {"tokens": tokens, "cotangent": cotangent, "piece_starts": piece_starts, "w_query": w_query, "w_key": w_key, "w_value": w_value, "w_out": w_out, "w_gate": w_gate, "w_up": w_up, "w_down": w_down, "attn_pre_gain": attn_pre_gain, "query_gain": query_gain, "key_gain": key_gain, "attn_post_gain": attn_post_gain, "mlp_pre_gain": mlp_pre_gain, "mlp_post_gain": mlp_post_gain}


@jax.custom_vjp
def low(v):
    return lax.optimization_barrier(v.astype(jnp.bfloat16)).astype(jnp.float32)

@jax.custom_vjp
def low_back(v):
    return v

def low_keep(v):
    return (low(v), None)

def low_pass(kept, grad):
    return (grad,)

def back_keep(v):
    return (v, None)

def back_low(kept, grad):
    return (low(grad),)
low.defvjp(low_keep, low_pass)
low_back.defvjp(back_keep, back_low)
epsilon = 1e-06
rope_base = 1000000.0
masked_value = -1e+30
per_group = 4

def normed(values, gain):
    return values * lax.rsqrt(lax.optimization_barrier(jnp.mean(values * values, axis=-1, keepdims=True)) + epsilon) * gain

def matmul(left, right):
    return jnp.einsum('gtd,df->gtf', left, right, precision=lax.Precision.HIGHEST)

def rope_tables(length, width):
    positions = jnp.arange(length, dtype=jnp.float32)
    freqs = rope_base ** (-jnp.arange(width // 2, dtype=jnp.float32) * 2.0 / width)
    angles = positions[:, None] * freqs[None, :]
    return (jnp.cos(angles), jnp.sin(angles))

def rotate(values, cosine, sine):
    half = values.shape[-1] // 2
    first = values[..., :half]
    second = values[..., half:]
    return jnp.concatenate([first * cosine - second * sine, second * cosine + first * sine], axis=-1)

def score_mask(rows, columns, starts):
    inside_rows = (rows[None, :] >= starts[:, None]) & (rows[None, :] < starts[:, None] + PIECE)
    inside_cols = (columns[None, :] >= starts[:, None]) & (columns[None, :] < starts[:, None] + PIECE)
    same = jnp.any(inside_rows[:, :, None] & inside_cols[:, None, :], axis=0)
    return (columns[None, :] <= rows[:, None]) | same

def forward(inputs, weights, starts):
    w_query, w_key, w_value, w_out, w_gate, w_up, w_down, gain_attn_pre, gain_query, gain_key, gain_attn_post, gain_mlp_pre, gain_mlp_post = weights
    groups, length, width = inputs.shape
    index = jnp.arange(length, dtype=jnp.int32)
    allowed = jax.vmap(lambda row_starts: score_mask(index, index, row_starts))(starts)
    cosine, sine = rope_tables(length, HD)
    normed_attn = low(normed(inputs, gain_attn_pre))
    query_proj = low_back(matmul(normed_attn, w_query)).reshape(groups, length, H, HD)
    key_proj = low_back(matmul(normed_attn, w_key))
    value_proj = low_back(matmul(normed_attn, w_value))
    query = low(rotate(normed(query_proj, gain_query), cosine[:, None, :], sine[:, None, :]) * HD ** (-0.5))
    key = low(rotate(normed(key_proj, gain_key), cosine, sine))
    value = low(value_proj)
    scores = low_back(jnp.einsum('gthd,gsd->ghts', query, key, precision=lax.Precision.HIGHEST))
    scores = jnp.where(allowed[:, None], scores, masked_value)
    probs = low(jax.nn.softmax(scores, axis=-1))
    mixed = jnp.einsum('ghts,gsd->gthd', probs, value, precision=lax.Precision.HIGHEST)
    mixed = low(low_back(mixed.reshape(groups, length, H * HD)))
    attn_out = low_back(matmul(mixed, w_out))
    resid = inputs + normed(attn_out, gain_attn_post)
    normed_mlp = low(normed(resid, gain_mlp_pre))
    gate = low_back(matmul(normed_mlp, w_gate))
    upper = low_back(matmul(normed_mlp, w_up))
    hidden = low(jax.nn.gelu(gate, approximate=True) * upper)
    mlp_out = low_back(matmul(hidden, w_down))
    return resid + normed(mlp_out, gain_mlp_post)

def reference(tokens, cotangent, piece_starts, w_query, w_key, w_value, w_out, w_gate, w_up, w_down, attn_pre_gain, query_gain, key_gain, attn_post_gain, mlp_pre_gain, mlp_post_gain):
    weights = tuple((item.astype(jnp.float32) for item in (w_query, w_key, w_value, w_out, w_gate, w_up, w_down, attn_pre_gain, query_gain, key_gain, attn_post_gain, mlp_pre_gain, mlp_post_gain)))
    inputs = tokens.astype(jnp.float32).reshape(-1, per_group, TOK_DEV, D)
    grads_in = cotangent.astype(jnp.float32).reshape(-1, per_group, TOK_DEV, D)
    starts = piece_starts.reshape(-1, per_group, NPIECE)

    def step(totals, item):
        group_in, group_grad, group_starts = item

        def apply(values, *params):
            return forward(values, params, group_starts)
        outputs, pull = jax.vjp(apply, group_in, *weights)
        grads = pull(group_grad)
        totals = tuple((total + grad for total, grad in zip(totals, grads[1:])))
        return (totals, (outputs, grads[0]))
    zeros = tuple((jnp.zeros(item.shape, jnp.float32) for item in weights))
    totals, (outputs, input_grads) = lax.scan(step, zeros, (inputs, grads_in, starts))
    layer_out = outputs.reshape(TOKENS, D).astype(jnp.bfloat16)
    input_grad = input_grads.reshape(TOKENS, D)
    return (layer_out, input_grad, totals[0], totals[1], totals[2], totals[3], totals[4], totals[5], totals[6], totals[7], totals[8], totals[9], totals[10], totals[11], totals[12])
```

```python
import jax
import jax.numpy as jnp
from jax import lax
from jax.sharding import PartitionSpec as P

D = 1152
H = 4
HD = 256
FF = 6912
PIECE = 256

epsilon = 1e-06
rope_base = 1000000.0
masked_value = -1e30
f32 = jnp.float32
bf16 = jnp.bfloat16


def row_scale(values):
    return lax.rsqrt(jnp.mean(values * values, axis=-1, keepdims=True) + epsilon)


def norm_back(values, scale, gain, upstream):
    weighted = upstream * gain
    inner = jnp.mean(weighted * values, axis=-1, keepdims=True)
    grad_values = scale * weighted - values * (scale * scale * scale) * inner
    grad_gain = jnp.sum((upstream * values * scale).reshape(-1, values.shape[-1]), axis=0)
    return (grad_values, grad_gain)


def rope_tables(length, width):
    positions = jnp.arange(length, dtype=f32)
    freqs = rope_base ** (-jnp.arange(width // 2, dtype=f32) * 2.0 / width)
    angles = positions[:, None] * freqs[None, :]
    return (jnp.cos(angles), jnp.sin(angles))


def rotate(values, cosine, sine):
    half = values.shape[-1] // 2
    first = values[..., :half]
    second = values[..., half:]
    return jnp.concatenate(
        [first * cosine - second * sine, second * cosine + first * sine], axis=-1
    )


def rotate_back(upstream, cosine, sine):
    half = upstream.shape[-1] // 2
    first = upstream[..., :half]
    second = upstream[..., half:]
    return jnp.concatenate(
        [first * cosine + second * sine, second * cosine - first * sine], axis=-1
    )


def matmul(left, right):
    return jnp.dot(left, right, preferred_element_type=f32)


def matmul_back(left, right):
    return lax.dot_general(left, right, (((1,), (1,)), ((), ())), preferred_element_type=f32)


def matmul_grad(left, right):
    return lax.dot_general(left, right, (((0,), (0,)), ((), ())), preferred_element_type=f32)


def plane_dims(chips):
    return {8: (4, 2), 32: (8, 4)}.get(chips, (chips, 1))


class Group:
    def __init__(self, count):
        self.count = count
        self.nz, self.ny = plane_dims(count // 2)
        me = lax.axis_index("fsdp")
        self.r = lax.axis_index("replica")
        self.c = me % 2
        self.y = (me // 2) % self.ny
        self.z = me // (2 * self.ny)

    def move(self, value, dz, dy):
        pairs = []
        for z in range(self.nz):
            for y in range(self.ny):
                for c in range(2):
                    to = ((z + dz) % self.nz * self.ny + (y + dy) % self.ny) * 2 + c
                    pairs.append(((z * self.ny + y) * 2 + c, to))
        return lax.ppermute(value, "fsdp", pairs)

    def other_core(self, value):
        return lax.ppermute(value, "fsdp", [(i, i ^ 1) for i in range(self.count)])

    def other_replica(self, value):
        return lax.ppermute(value, "replica", [(0, 1), (1, 0)])

    def gather(self, block):
        buffer = jnp.zeros((self.nz, self.ny) + block.shape, block.dtype)
        for dz in range(self.nz):
            piece = block if dz == 0 else self.move(block, dz, 0)
            for dy in range(self.ny):
                part = piece if dy == 0 else self.move(piece, 0, dy)
                where = ((self.z - dz) % self.nz, (self.y - dy) % self.ny)
                buffer = lax.dynamic_update_slice(
                    buffer, part[None, None], where + (0,) * block.ndim
                )
        return buffer

    def scatter(self, blocks):
        def pick(dz, dy):
            where = ((self.z + dz) % self.nz, (self.y + dy) % self.ny)
            size = (1, 1) + blocks.shape[2:]
            return lax.dynamic_slice(blocks, where + (0,) * (blocks.ndim - 2), size)[0, 0]

        total = None
        for dz in list(range(1, self.nz)) + [0]:
            line = pick(dz, 0).astype(f32)
            for dy in range(1, self.ny):
                line = line + self.move(pick(dz, dy), 0, dy).astype(f32)
            if dz:
                line = self.move(line.astype(bf16), dz, 0).astype(f32)
            total = line if total is None else total + line
        return total

    def by_core(self, mine, theirs):
        first = jnp.where(self.c == 0, mine, theirs)
        second = jnp.where(self.c == 0, theirs, mine)
        return jnp.stack([first, second])

    def by_replica(self, mine, theirs):
        first = jnp.where(self.r == 0, mine, theirs)
        second = jnp.where(self.r == 0, theirs, mine)
        return jnp.stack([first, second])

    def share(self, rows):
        pair = jnp.concatenate([rows, self.other_replica(rows)], axis=0)
        return jnp.concatenate([pair, self.other_core(pair)], axis=0)

    def collect(self, partial):
        half = partial.shape[0] // 2
        pair = partial[:half] + self.other_core(partial[half:].astype(bf16)).astype(f32)
        quarter = half // 2
        return pair[:quarter] + self.other_replica(pair[quarter:].astype(bf16)).astype(f32)


def on_device(
    tokens,
    cotangent,
    piece_starts,
    w_query,
    w_key,
    w_value,
    w_out,
    w_gate,
    w_up,
    w_down,
    attn_pre_gain,
    query_gain,
    key_gain,
    attn_post_gain,
    mlp_pre_gain,
    mlp_post_gain,
):
    length = tokens.shape[0]
    count = lax.axis_size("fsdp")
    group = Group(count)
    chips = count // 2
    d_rows = D // count
    g_rows = HD // count
    o_rows = H * HD // count
    sub = FF // count // 2
    quarter = chips * sub
    qwidth = H * HD
    inner = qwidth + 2 * HD

    gain_block = jnp.zeros((d_rows, 128), bf16)
    for column, gain in enumerate(
        (attn_pre_gain, attn_post_gain, mlp_pre_gain, mlp_post_gain, query_gain, key_gain)
    ):
        gain_block = lax.dynamic_update_slice(gain_block, gain[:, None], (0, column))
    attn_block = jnp.concatenate([w_query, w_key, w_value, gain_block], axis=1)
    attn_core = group.gather(attn_block)
    attn_pairs = group.by_core(attn_core, group.other_core(attn_core))
    attn_all = attn_pairs.transpose(1, 2, 0, 3, 4).reshape(D, inner + 128)
    out_core = group.gather(w_out)
    out_pairs = group.by_core(out_core, group.other_core(out_core))
    w_out_all = out_pairs.transpose(1, 2, 0, 3, 4).reshape(qwidth, D)
    w_qkv = attn_all[:, :inner]
    gains = attn_all[:, inner : inner + 8].astype(f32).T
    gain_attn_pre, gain_attn_post, gain_mlp_pre, gain_mlp_post = (gains[i] for i in range(4))
    head_gains = gains[4:6].reshape(2, count, d_rows)[:, :, :g_rows].reshape(2, HD)
    gain_query, gain_key = head_gains[0], head_gains[1]

    def column_quarter(weight):
        pieces = weight.reshape(d_rows, chips, 2, 2, sub)

        def take(core):
            piece = lax.dynamic_slice(
                pieces, (0, 0, core, group.r, 0), (d_rows, chips, 1, 1, sub)
            )
            return piece.reshape(d_rows, quarter)

        mine = take(group.c)
        return group.by_core(mine, group.other_core(take(1 - group.c)))

    w_gate_q = group.gather(column_quarter(w_gate)).reshape(D, quarter)
    w_up_q = group.gather(column_quarter(w_up)).reshape(D, quarter)
    down_half = lax.dynamic_slice(w_down, (group.r * sub, 0), (sub, D))
    w_down_q = group.gather(down_half).reshape(quarter, D)

    inputs = tokens.astype(f32)
    scale_attn = row_scale(inputs)
    normed_attn = (inputs * scale_attn * gain_attn_pre).astype(bf16)
    projected = matmul(normed_attn, w_qkv)
    query_proj = projected[:, :qwidth].reshape(length, H, HD)
    key_proj = projected[:, qwidth : qwidth + HD]
    value_low = projected[:, qwidth + HD :].astype(bf16)
    cosine, sine = rope_tables(length, HD)
    attn_factor = HD ** (-0.5)
    scale_query = row_scale(query_proj)
    query_low = (
        rotate(query_proj * scale_query * gain_query, cosine[:, None, :], sine[:, None, :])
        * attn_factor
    ).astype(bf16)
    scale_key = row_scale(key_proj)
    key_low = rotate(key_proj * scale_key * gain_key, cosine, sine).astype(bf16)
    rows = jnp.arange(length, dtype=jnp.int32)
    allowed = rows[None, :] <= rows[:, None]
    for piece in range(piece_starts.shape[1]):
        start = piece_starts[0, piece]
        inside = (rows >= start) & (rows < start + PIECE)
        allowed = allowed | (inside[:, None] & inside[None, :])
    scores = jnp.einsum("thd,sd->hts", query_low, key_low, preferred_element_type=f32)
    scores = jnp.where(allowed[None], scores, masked_value)
    peak = jnp.max(scores, axis=-1, keepdims=True)
    expo = jnp.exp(scores - peak)
    total = jnp.sum(expo, axis=-1, keepdims=True)
    probs = expo / total
    probs_low = probs.astype(bf16)
    mixed = jnp.einsum("hts,sd->thd", probs_low, value_low, preferred_element_type=f32)
    mixed_low = mixed.reshape(length, qwidth).astype(bf16)
    attn_out = matmul(mixed_low, w_out_all)
    scale_post = row_scale(attn_out)
    resid = inputs + attn_out * scale_post * gain_attn_post

    scale_mlp = row_scale(resid)
    normed_mlp = (resid * scale_mlp * gain_mlp_pre).astype(bf16)
    normed_all = group.share(normed_mlp)
    gate = matmul(normed_all, w_gate_q)
    upper = matmul(normed_all, w_up_q)
    activated, gelu_pull = jax.vjp(lambda values: jax.nn.gelu(values, approximate=True), gate)
    hidden_low = (activated * upper).astype(bf16)
    mlp_out = group.collect(matmul(hidden_low, w_down_q))
    scale_out = row_scale(mlp_out)
    layer_out = (resid + mlp_out * scale_out * gain_mlp_post).astype(bf16)

    upstream = cotangent.astype(f32)
    grad_mlp_out, grad_mlp_post = norm_back(mlp_out, scale_out, gain_mlp_post, upstream)
    grad_mlp_all = group.share(grad_mlp_out.astype(bf16))
    grad_hidden = matmul_back(grad_mlp_all, w_down_q)
    grad_gate_low = gelu_pull(grad_hidden * upper)[0].astype(bf16)
    grad_up_low = (grad_hidden * activated).astype(bf16)
    down_share = group.scatter(
        matmul_grad(hidden_low, grad_mlp_all)
        .astype(bf16)
        .reshape(group.nz, group.ny, sub, D)
    )
    grad_normed_mlp = group.collect(
        matmul_back(grad_gate_low, w_gate_q) + matmul_back(grad_up_low, w_up_q)
    )

    def column_share(grads):
        share = group.scatter(
            matmul_grad(normed_all, grads)
            .astype(bf16)
            .reshape(group.nz, group.ny, 2, d_rows, quarter)
        ).astype(bf16)
        mine = lax.dynamic_index_in_dim(share, group.c, 0, keepdims=False)
        theirs = lax.dynamic_index_in_dim(share, 1 - group.c, 0, keepdims=False)
        cores = group.by_core(mine, group.other_core(theirs))
        both = group.by_replica(cores, group.other_replica(cores))
        pieces = both.reshape(2, 2, d_rows, chips, sub).transpose(2, 3, 1, 0, 4)
        return pieces.reshape(d_rows, FF).astype(f32)

    grad_gate = column_share(grad_gate_low)
    grad_up = column_share(grad_up_low)
    down_low = down_share.astype(bf16)
    grad_down = (
        group.by_replica(down_low, group.other_replica(down_low)).reshape(2 * sub, D).astype(f32)
    )

    grad_resid_part, grad_mlp_pre = norm_back(resid, scale_mlp, gain_mlp_pre, grad_normed_mlp)
    grad_resid = upstream + grad_resid_part
    grad_attn_out, grad_attn_post = norm_back(attn_out, scale_post, gain_attn_post, grad_resid)
    grad_attn_low = grad_attn_out.astype(bf16)

    def both_sum(terms, rows_each):
        blocks = terms.astype(bf16).reshape(group.nz, group.ny, 2, rows_each, -1)
        mine = lax.dynamic_index_in_dim(blocks, group.c, 2, keepdims=False)
        theirs = lax.dynamic_index_in_dim(blocks, 1 - group.c, 2, keepdims=False)
        blocks = (mine.astype(f32) + group.other_core(theirs).astype(f32)).astype(bf16)
        share = group.scatter(blocks).astype(bf16)
        return share.astype(f32) + group.other_replica(share).astype(f32)

    grad_out = both_sum(matmul_grad(mixed_low, grad_attn_low), o_rows)
    grad_mixed = matmul_back(grad_attn_low, w_out_all).astype(bf16).reshape(length, H, HD)
    grad_probs = jnp.einsum("thd,sd->hts", grad_mixed, value_low, preferred_element_type=f32)
    grad_value_act = jnp.einsum(
        "hts,thd->sd", probs_low, grad_mixed, preferred_element_type=f32
    )
    inner_sum = jnp.sum(probs * grad_probs, axis=-1, keepdims=True)
    grad_scores = (probs * (grad_probs - inner_sum)).astype(bf16)
    grad_query_act = jnp.einsum("hts,sd->thd", grad_scores, key_low, preferred_element_type=f32)
    grad_key_rot = jnp.einsum("hts,thd->sd", grad_scores, query_low, preferred_element_type=f32)
    grad_query_normed = rotate_back(
        grad_query_act * attn_factor, cosine[:, None, :], sine[:, None, :]
    )
    grad_query_proj, grad_query_gain = norm_back(
        query_proj, scale_query, gain_query, grad_query_normed
    )
    grad_key_normed = rotate_back(grad_key_rot, cosine, sine)
    grad_key_proj, grad_key_gain = norm_back(key_proj, scale_key, gain_key, grad_key_normed)
    grad_qkv_low = jnp.concatenate(
        [grad_query_proj.reshape(length, qwidth), grad_key_proj, grad_value_act], axis=1
    ).astype(bf16)
    grad_normed_attn = matmul_back(grad_qkv_low, w_qkv)
    grad_input_part, grad_attn_pre = norm_back(inputs, scale_attn, gain_attn_pre, grad_normed_attn)
    input_grad = grad_resid + grad_input_part
    head_columns = jnp.stack([grad_query_gain, grad_key_gain], axis=1).reshape(count, g_rows, 2)
    head_columns = jnp.pad(head_columns, ((0, 0), (0, d_rows - g_rows), (0, 0))).reshape(D, 2)
    gain_columns = jnp.concatenate(
        [
            jnp.stack([grad_attn_pre, grad_attn_post, grad_mlp_pre, grad_mlp_post], axis=1),
            head_columns,
            jnp.zeros((D, 122), f32),
        ],
        axis=1,
    )
    attn_sum = both_sum(
        jnp.concatenate([matmul_grad(normed_attn, grad_qkv_low), gain_columns], axis=1), d_rows
    )
    gain_sum = attn_sum[:, inner : inner + 8].T
    return (
        layer_out,
        input_grad,
        attn_sum[:, :qwidth],
        attn_sum[:, qwidth : qwidth + HD],
        attn_sum[:, qwidth + HD : inner],
        grad_out,
        grad_gate,
        grad_up,
        grad_down,
        gain_sum[0],
        gain_sum[4, :g_rows],
        gain_sum[5, :g_rows],
        gain_sum[1],
        gain_sum[2],
        gain_sum[3],
    )


def solution(mesh):
    rows = P(("replica", "fsdp"), None)
    weight = P("fsdp", None)
    gain = P("fsdp")
    return jax.shard_map(
        on_device,
        mesh=mesh,
        in_specs=(rows,) * 3 + (weight,) * 7 + (gain,) * 6,
        out_specs=(rows,) * 2 + (weight,) * 7 + (gain,) * 6,
        check_vma=False,
    )
```
